32 devices in a mesh: dp: 8 (over z, y), blk: 4 (over x, core).
Axes of the slice: x: 2, y: 2, z: 4, core: 2. Of those that a mesh axis runs over, the one named last changes fastest.
Arguments:
- tokens: bfloat16 [4096, 4096], P(('dp', 'blk')), may hold values from -6 to 6
- gate_projection_weight: bfloat16 [4096, 7168], P(None, 'blk'), may hold values from -0.09375 to 0.09375
- up_projection_weight: bfloat16 [4096, 7168], P('dp', 'blk'), may hold values from -0.09375 to 0.09375
- down_projection_weight: bfloat16 [7168, 4096], P('blk', 'dp'), may hold values from -0.0625 to 0.0625
- router_projection_weight: bfloat16 [4096, 8], replicated, may hold values from -0.09375 to 0.09375
- adapter_down_factors: bfloat16 [4096, 128], replicated, may hold values from -0.09375 to 0.09375
- adapter_up_factors: bfloat16 [128, 4096], replicated, may hold values from -1.5 to 1.5
- routes: int32 [4096, 2], P(('dp', 'blk')), may hold values from 0 to 7, all different within a row
- padding_token_mask: int32 [4096], P(('dp', 'blk')), may hold values 0 or 1
- cotangent: bfloat16 [4096, 4096], P(('dp', 'blk')), may hold values from -6 to 6
Outputs:
- layer_out: bfloat16 [4096, 4096], P(('dp', 'blk'))
- grad_down: float32 [4096, 128], replicated
- grad_up: float32 [128, 4096], replicated
The draws below stay inside these ranges and needn't reach their ends.
Inputs may be any that keep to these rules, and one draw needn't show every extreme that they name: `routes`: the two experts of a token differ.
All inputs are finite; a program needn't handle non-finite values. No bound on the sum of `padding_token_mask` on one device may be relied on, other than what follows from the above.
Results may differ from the reference program's by a relative error of at most 0.0075.
Values may be sent and summed in bfloat16 or wider, within the bound.
A program may use at most 192 MiB of HBM per device.

```python
import jax
import jax.numpy as jnp
from jax import lax

MODEL_WIDTH = 4096
FF = 7168
EXPERTS = 8
EXPERT_RANK = 16
TOKENS = 4096
LOW_RANK_COLUMNS = 128
N_BLK = 4


def place_ends(result, own_key, least, top_value):
    spot = [jax.random.randint(jax.random.fold_in(own_key, axis), (), 0, length) for axis, length in enumerate(result.shape)]
    longest = result.shape.index(max(result.shape))
    beside = spot[:longest] + [(spot[longest] + 1) % result.shape[longest]] + spot[longest + 1:]
    return result.at[tuple(spot)].set(least).at[tuple(beside)].set(top_value)


def shard_levels(own_key, shape, shards, low, top_value):
    loudness, own = 1.0, jax.random.fold_in(own_key, 6)
    for dim, blocks in shards:
        draws = jnp.exp(jax.random.uniform(jax.random.fold_in(own, dim), (blocks,), jnp.float32, low / len(shards), top_value / len(shards)))
        loudness = loudness * jnp.repeat(draws, shape[dim] // blocks).reshape([-1 if axis == dim else 1 for axis in range(len(shape))])
    return loudness


def choose_distinct(rng, rows, count, top, lift):
    order = jax.random.permutation(jax.random.fold_in(rng, 1), count)
    boost = order
    for power in range(3):
        boost = boost * boost // count
    boost = boost * lift // count
    chance = jax.random.randint(jax.random.fold_in(rng, 2), (rows, count), 0, 4096) + boost
    holders = jax.random.permutation(jax.random.fold_in(rng, 3), rows)[jnp.arange(count) % rows]
    chance = jnp.where(jnp.arange(rows)[:, None] == holders[None, :], 1 << 14, chance)
    merit = chance * count + jnp.arange(count)
    return lax.top_k(merit.astype(jnp.int32), top)[1].astype(jnp.int32)


def centred(stream_key, extent, scale, most, shards=(), kind=jnp.bfloat16):
    level = shard_levels(stream_key, extent, shards, -0.22, 0.18) if shards else 1.0
    array = jax.random.normal(stream_key, extent, jnp.float32) * scale * level
    return jnp.minimum(jnp.maximum(array, -most), most).astype(kind)


def setup_inputs(seed: int = 0) -> dict:
    splits = jax.random.split(jax.random.key(seed), 11)
    return {
        "tokens": centred(splits[0], (TOKENS, MODEL_WIDTH), 1.0, 6.0, ((0, 32),)),
        "gate_projection_weight": centred(splits[1], (MODEL_WIDTH, FF), MODEL_WIDTH ** -0.5, 0.09375, ((1, 4),)),
        "up_projection_weight": centred(splits[2], (MODEL_WIDTH, FF), MODEL_WIDTH ** -0.5, 0.09375, ((0, 8), (1, 4))),
        "down_projection_weight": centred(splits[3], (FF, MODEL_WIDTH), FF ** -0.5, 0.0625, ((0, 4), (1, 8))),
        "router_projection_weight": centred(splits[4], (MODEL_WIDTH, EXPERTS), MODEL_WIDTH ** -0.5, 0.09375),
        "adapter_down_factors": centred(splits[5], (MODEL_WIDTH, LOW_RANK_COLUMNS), MODEL_WIDTH ** -0.5, 0.09375),
        "adapter_up_factors": centred(splits[6], (LOW_RANK_COLUMNS, MODEL_WIDTH), EXPERT_RANK ** -0.5, 1.5),
        "routes": choose_distinct(splits[7], TOKENS, EXPERTS, 2, 2048),
        "padding_token_mask": place_ends((jax.random.randint(splits[8], (TOKENS,), 0, 8) < 7).astype(jnp.int32), jax.random.fold_in(splits[8], 1), 0, 1),
        "cotangent": centred(splits[9], (TOKENS, MODEL_WIDTH), 1.0, 6.0, ((0, 32),)),
    }


def reference(tokens, gate_projection_weight, up_projection_weight, down_projection_weight, router_projection_weight, adapter_down_factors, adapter_up_factors, routes, padding_token_mask, cotangent):
    width = FF // N_BLK
    base = jnp.zeros((tokens.shape[0], tokens.shape[1]), jnp.float32)
    for group in range(N_BLK):
        lower = group * width
        gate_act = jnp.dot(tokens, gate_projection_weight[:, lower:lower + width], preferred_element_type=jnp.float32)
        up_act = jnp.dot(tokens, up_projection_weight[:, lower:lower + width], preferred_element_type=jnp.float32)
        hidden = (jax.nn.silu(gate_act) * up_act).astype(jnp.bfloat16)
        part = jnp.dot(hidden, down_projection_weight[lower:lower + width, :], preferred_element_type=jnp.float32)
        part = lax.optimization_barrier(part.astype(jnp.bfloat16))
        base = base + part.astype(jnp.float32)
    logits = jnp.dot(tokens, router_projection_weight, preferred_element_type=jnp.float32)
    experts_iota = jnp.arange(EXPERTS, dtype=jnp.int32)[None, :]
    first_hot = (routes[:, 0:1] == experts_iota).astype(jnp.float32)
    second_hot = (routes[:, 1:2] == experts_iota).astype(jnp.float32)
    first_logit = jnp.sum(logits * first_hot, axis=1, keepdims=True)
    second_logit = jnp.sum(logits * second_hot, axis=1, keepdims=True)
    weight_first = jax.nn.sigmoid(first_logit - second_logit)
    coeff = weight_first * first_hot + (1.0 - weight_first) * second_hot
    coeff_wide = jnp.repeat(coeff, EXPERT_RANK, axis=1)
    low_rank_state = jnp.dot(tokens, adapter_down_factors, preferred_element_type=jnp.float32)
    scaled_output = (low_rank_state * coeff_wide).astype(jnp.bfloat16)
    adapter_delta = jnp.dot(scaled_output, adapter_up_factors, preferred_element_type=jnp.float32)
    layer_out = (base + adapter_delta).astype(jnp.bfloat16)
    masked_tokens = cotangent * padding_token_mask[:, None].astype(jnp.bfloat16)
    low_rank_gradient = lax.dot_general(masked_tokens, adapter_up_factors, (((1,), (1,)), ((), ())), preferred_element_type=jnp.float32)
    dlow = (low_rank_gradient * coeff_wide).astype(jnp.bfloat16)
    live = jnp.sum(padding_token_mask.astype(jnp.float32))
    inverse = 1.0 / jnp.maximum(live, 1.0)
    grad_up = lax.dot_general(scaled_output, masked_tokens, (((0,), (0,)), ((), ())), preferred_element_type=jnp.float32) * inverse
    grad_down = lax.dot_general(tokens, dlow, (((0,), (0,)), ((), ())), preferred_element_type=jnp.float32) * inverse
    return layer_out, grad_down, grad_up
```

```python
import jax
import jax.numpy as jnp
from jax import lax
from jax.sharding import PartitionSpec as P


CHUNKS = 2
F32 = jnp.float32
BF16 = jnp.bfloat16


def flip(value, n, mask):
    return lax.ppermute(value, "dp", [(d, d ^ mask) for d in range(n)])


def gather_half(block, n, bits):
    held = {0: block}
    for bit in bits:
        held.update({mask ^ bit: flip(value, n, bit) for mask, value in list(held.items())})
    return held


def shards(
    n,
    tokens,
    gate_projection_weight,
    up_projection_weight,
    down_projection_weight,
    router_projection_weight,
    adapter_down_factors,
    adapter_up_factors,
    routes,
    padding_token_mask,
    cotangent,
):
    half = n // 2
    me = lax.axis_index("dp")
    top, low = me // half, me % half
    bits = [1 << b for b in range(half.bit_length() - 1)]
    owned, width = tokens.shape
    rows = up_projection_weight.shape[0]
    out_columns = down_projection_weight.shape[1]
    hidden_units = up_projection_weight.shape[1]
    chunk = hidden_units // CHUNKS
    half_width = half * rows

    away = flip(
        lax.dynamic_slice(tokens, (0, (1 - top) * half_width), (owned, half_width)), n, half
    )
    grouped = lax.all_gather(tokens, "blk", axis=0, tiled=True)
    away = lax.all_gather(away, "blk", axis=0, tiled=True)

    up_blocks = [
        gather_half(
            up_projection_weight[:, c * chunk : (c + 1) * chunk], n, bits if c % 2 == 0 else bits[::-1]
        )
        for c in range(CHUNKS)
    ]
    last = [up_blocks[c][half - 1] for c in range(CHUNKS)]
    down, last = lax.optimization_barrier((down_projection_weight, last))
    for c in range(CHUNKS):
        up_blocks[c][half - 1] = last[c]
    down_blocks = [
        gather_half(
            down[c * chunk : (c + 1) * chunk], n, bits if c % 2 == 0 else bits[::-1]
        )
        for c in range(CHUNKS)
    ]

    gate_act = jnp.dot(grouped, gate_projection_weight, preferred_element_type=F32)

    def up_sum(c, values, base):
        total = 0.0
        for mask in range(half):
            piece = lax.dynamic_slice(
                values, (0, base + (low ^ mask) * rows), (values.shape[0], rows)
            )
            total += jnp.dot(piece, up_blocks[c][mask], preferred_element_type=F32)
        return total

    sent = [flip(up_sum(c, away, 0).astype(BF16), n, half) for c in range(CHUNKS)]
    hidden, hidden_away = [], []
    for c in range(CHUNKS):
        up_act = up_sum(c, grouped, top * half_width) + sent[c].astype(F32)
        gate = gate_act[:, c * chunk : (c + 1) * chunk]
        hidden.append((jax.nn.silu(gate) * up_act).astype(BF16))
        hidden_away.append(flip(hidden[c], n, half))

    def part_of(values):
        columns = []
        for mask in range(half):
            total = 0.0
            for c in range(CHUNKS):
                total += jnp.dot(values[c], down_blocks[c][mask], preferred_element_type=F32)
            columns.append(total.astype(BF16))
        part = jnp.concatenate(columns, axis=1)
        return lax.psum_scatter(part, "blk", scatter_dimension=0, tiled=True)

    base_near = part_of(hidden)
    base_far = flip(part_of(hidden_away), n, half)

    def in_order(value):
        return [
            lax.dynamic_slice(value, (0, (low ^ p) * out_columns), (owned, out_columns))
            for p in range(half)
        ]

    near = jnp.concatenate(in_order(base_near), axis=1)
    far = jnp.concatenate(in_order(base_far), axis=1)
    base = jnp.where(
        top == 0, jnp.concatenate([near, far], axis=1), jnp.concatenate([far, near], axis=1)
    ).astype(F32)

    expert_list = router_projection_weight.shape[1]
    rank_index = adapter_down_factors.shape[1] // expert_list
    logits = jnp.dot(tokens, router_projection_weight, preferred_element_type=F32)
    experts_iota = jnp.arange(expert_list, dtype=jnp.int32)[None, :]
    first_hot = (routes[:, 0:1] == experts_iota).astype(F32)
    second_hot = (routes[:, 1:2] == experts_iota).astype(F32)
    first_logit = jnp.sum(logits * first_hot, axis=1, keepdims=True)
    second_logit = jnp.sum(logits * second_hot, axis=1, keepdims=True)
    weight_first = jax.nn.sigmoid(first_logit - second_logit)
    coeff = weight_first * first_hot + (1.0 - weight_first) * second_hot
    coeff_wide = jnp.repeat(coeff, rank_index, axis=1)
    low_rank_state = jnp.dot(tokens, adapter_down_factors, preferred_element_type=F32)
    scaled_output = (low_rank_state * coeff_wide).astype(BF16)
    adapter_delta = jnp.dot(scaled_output, adapter_up_factors, preferred_element_type=F32)
    layer_out = (base + adapter_delta).astype(BF16)
    masked_tokens = cotangent * padding_token_mask[:, None].astype(BF16)
    low_rank_gradient = lax.dot_general(
        masked_tokens,
        adapter_up_factors,
        (((1,), (1,)), ((), ())),
        preferred_element_type=F32,
    )
    dlow = (low_rank_gradient * coeff_wide).astype(BF16)
    local_live = jnp.sum(padding_token_mask.astype(F32))
    local_up = lax.dot_general(
        scaled_output, masked_tokens, (((0,), (0,)), ((), ())), preferred_element_type=F32
    )
    local_down = lax.dot_general(
        tokens, dlow, (((0,), (0,)), ((), ())), preferred_element_type=F32
    )
    summed_down, summed_up, live_total = lax.psum((local_down, local_up, local_live), ("dp", "blk"))
    inverse = 1.0 / jnp.maximum(live_total, 1.0)
    grad_down = summed_down * inverse
    grad_up = summed_up * inverse
    return (layer_out, grad_down, grad_up)


def solution(mesh):
    n = mesh.shape["dp"]

    def run(*args):
        return shards(n, *args)

    return jax.shard_map(
        run,
        mesh=mesh,
        in_specs=(
            P(("dp", "blk"), None),
            P(None, "blk"),
            P("dp", "blk"),
            P("blk", "dp"),
            P(),
            P(),
            P(),
            P(("dp", "blk"), None),
            P(("dp", "blk")),
            P(("dp", "blk"), None),
        ),
        out_specs=(P(("dp", "blk"), None), P(), P()),
        check_vma=False,
    )
```
